32 devices in a mesh: grp: 2 (over y), shard: 8 (over z, x), rep: 2 (over core).
Axes of the slice: x: 2, y: 2, z: 4, core: 2. Of those that a mesh axis runs over, the one named last changes fastest.
Arguments:
- replica_weights: bfloat16 [4, 4096, 14336], P(('grp', 'rep'), None, 'shard'), parts along dimension 0, may hold values from -6 to 6
- global_weights: float32 [8192, 14336], P(('grp', 'shard', 'rep')), parts along dimension 0, may hold values from -6 to 6
- momentum: float32 [8192, 14336], P(('grp', 'shard', 'rep')), parts along dimension 0, may hold values from -3 to 3
Outputs:
- new_params: bfloat16 [8192, 14336], P('grp', 'shard'), parts along dimension 0
- new_global: float32 [8192, 14336], P(('grp', 'shard', 'rep')), parts along dimension 0
- new_momentum: float32 [8192, 14336], P(('grp', 'shard', 'rep')), parts along dimension 0
The draws below stay inside these ranges and needn't reach their ends.
There are 2 independent parts, one for each index of `grp`. The reference program is written for one: setup_inputs(seed, part) draws one part's arguments, and reference() takes and returns one part's arrays. A program takes and returns all parts, laid end to end along the dimension named above; each array names one. Nothing has to cross between parts.
All inputs are finite; a program needn't handle non-finite values.
Results may differ from the reference program's by a relative error of at most 0.008.
Values may be sent and summed in bfloat16 or wider, within the bound.
No kernel may reach another device: no remote copies, remote signals or barrier semaphores. Data moves between devices by JAX's collectives and lax.ppermute only.
A program may use at most 192 MiB of HBM per device.

```python
import jax
import jax.numpy as jnp

D = 4096
FF = 14336
REPLICAS = 2


def block_scale(rng, extent, pieces, smallest, top_value):
    loudness, own = 1.0, jax.random.fold_in(rng, 6)
    for position, parts in pieces:
        draws = jnp.exp(jax.random.uniform(jax.random.fold_in(own, position), (parts,), jnp.float32, smallest / len(pieces), top_value / len(pieces)))
        loudness = loudness * jnp.repeat(draws, extent[position] // parts).reshape([-1 if axis == position else 1 for axis in range(len(extent))])
    return loudness


def scatter_about(key, extent, spread, reach, cuts=(), dtype=jnp.bfloat16):
    array = jax.random.normal(key, extent, jnp.float32) * spread
    if len(cuts) > 0:
        array = block_scale(key, extent, cuts, -0.22, 0.18) * array
    return jnp.clip(array, min=-reach, max=reach).astype(dtype)


def setup_inputs(seed: int = 0, part: int = 0) -> dict:
    seeds = jax.random.split(jax.random.key(seed), 4)
    own_keys = jax.random.split(jax.random.fold_in(seeds[3], part), 4)
    replica_weights = scatter_about(own_keys[0], (REPLICAS, D, FF), 1.0, 6.0, ((0, 2), (2, 8)))
    global_weights = scatter_about(own_keys[1], (D, FF), 1.0, 6.0, ((0, 16),), jnp.float32)
    momentum = scatter_about(own_keys[2], (D, FF), 0.5, 3.0, ((0, 16),), jnp.float32)
    return dict(replica_weights=replica_weights, global_weights=global_weights, momentum=momentum)


outer_rate = 0.7
momentum_decay = 0.9


def reference(replica_weights, global_weights, momentum):
    total = jnp.sum(replica_weights.astype(jnp.float32), axis=0)
    delta = global_weights - total / jnp.float32(REPLICAS)
    new_momentum = momentum_decay * momentum + delta
    new_global = global_weights - outer_rate * (delta + momentum_decay * new_momentum)
    new_params = new_global.astype(jnp.bfloat16)
    return (new_params, new_global, new_momentum)
```

```python
import functools
import math

import jax
import jax.numpy as jnp
from jax import lax
from jax.experimental import pallas as pl
from jax.experimental.pallas import tpu as pltpu
from jax.sharding import PartitionSpec as P


outer_rate = 0.7
momentum_decay = 0.9


def call(kernel, place, ins, in_maps, outs, out_maps, tile, width, grid, aliases, bytes_moved):
    any_space = pl.BlockSpec(memory_space=pl.ANY)
    return pl.pallas_call(
        kernel,
        grid_spec=pltpu.PrefetchScalarGridSpec(
            num_scalar_prefetch=1,
            grid=grid,
            in_specs=[any_space if m is None else pl.BlockSpec((tile, width), m) for m in in_maps],
            out_specs=[pl.BlockSpec((tile, width), m) for m in out_maps],
        ),
        out_shape=outs,
        input_output_aliases=aliases,
        compiler_params=pltpu.CompilerParams(vmem_limit_bytes=48 * 1024 * 1024),
        cost_estimate=pl.CostEstimate(flops=bytes_moved, bytes_accessed=bytes_moved, transcendentals=0),
    )(place, *ins)


def back_term_kernel(place, weights, momentum, out):
    keep = 1.0 - outer_rate * (1.0 + momentum_decay)
    carry = outer_rate * momentum_decay * momentum_decay
    out[...] = (keep * weights[...] - carry * momentum[...]).astype(out.dtype)


def sum_kernel(place, mine, theirs, out):
    out[...] = (mine[...].astype(jnp.float32) + theirs[...].astype(jnp.float32)).astype(out.dtype)


def fresh_kernel(place, mine, theirs, back, other, *rest, replicas):
    out = rest[-1]
    share = outer_rate * (1.0 + momentum_decay) / replicas
    total = mine[...].astype(jnp.float32) + theirs[...].astype(jnp.float32)
    first = pl.program_id(0) == 0
    term = jnp.where(first, back[...].astype(jnp.float32), other[...].astype(jnp.float32))
    out[...] = (share * total + term).astype(out.dtype)


def update_kernel(place, total, weights, momentum, *rest, replicas):
    new_weights, new_momentum = rest[-2:]
    old = weights[...]
    delta = old - total[...].astype(jnp.float32) * (1.0 / replicas)
    moved = momentum_decay * momentum[...] + delta
    new_momentum[...] = moved
    new_weights[...] = old - outer_rate * (delta + momentum_decay * moved)


def offsets(shards):
    half = shards // 2
    order, top = [], half // 2
    while top:
        lines = range(2 * top - 1, top - 1, -1)
        order += [2 * j for j in lines] + [2 * j + 1 for j in lines]
        top //= 2
    return order + [1]


def cut(k, owned, sizes):
    unit, out, row = owned // 16, [], 0
    for part, size in enumerate(sizes):
        out.append((k, row, size * unit, part))
        row += size * unit
    return out


def plan(shards, owned):
    order = offsets(shards)
    far = [k for k in order if k >= shards // 2]
    near = [k for k in reversed(order) if k < shards // 2]
    half = len(far) // 2
    late = far[:half] + far[half:][::-1]
    backs = {k: cut(k, owned, first_cut if k == order[0] else (16,)) for k in order}
    totals = {k: cut(k, owned, last_cut if k == late[-1] else (16,)) for k in order}
    flat = lambda pieces, ks: [p for k in ks for p in pieces[k]]
    return (
        flat(backs, order), flat(totals, late + [k for k in order if k not in far]),
        flat(backs, far[:half] + near + far[half:]), flat(totals, near + late),
    )


first_cut = (4, 12)
last_cut = (8, 8)


def pipelined(local, weights, momentum):
    rows, width = local.shape
    shards = lax.axis_size("shard")
    pairs = lax.axis_size("rep")
    owned = weights.shape[0]
    me = lax.axis_index("shard")
    core = lax.axis_index("rep")

    def swap(x):
        return lax.ppermute(x, "rep", [(i, i ^ 1) for i in range(pairs)])

    def send(x, k):
        return lax.ppermute(x, "shard", [(i, i ^ k) for i in range(shards)])

    def scalars(*values):
        return jnp.stack([jnp.asarray(v, jnp.int32) for v in values])

    def geometry(piece, largest):
        k, row, count, _ = piece
        tile = math.gcd(math.gcd(row, count), largest)
        return k, row // tile, count // tile, owned // tile, tile, count * width

    def block(piece):
        return (jax.ShapeDtypeStruct((piece[2], width), local.dtype),)

    plain = lambda i, p: (i, 0)

    def back_term(piece):
        k, skip, steps, _, tile, area = geometry(piece, 128)
        column = lambda i, p: (skip + i, p[0])
        return call(
            back_term_kernel, scalars(me ^ k), (weights, momentum), (column, column),
            block(piece), (plain,), tile, width, (steps,), {}, 10 * area)[0]

    def sum_block(piece, theirs):
        k, skip, steps, per, tile, area = geometry(piece, 128)
        rowed = lambda i, p: (p[0] * per + skip + i, 0)
        return call(
            sum_kernel, scalars((me ^ k) * pairs + core), (local, theirs), (rowed, rowed),
            block(piece), (plain,), tile, width, (steps,), {}, 6 * area)[0]

    def fresh_block(piece, theirs, back, other, out):
        k, skip, steps, per, tile, area = geometry(piece, owned)
        halves = lambda h, i, p: ((p[0] ^ h) * per + skip + i, 0)
        inner = lambda h, i, p: (i, 0)
        ins, maps = [local, theirs, back, other], [halves, halves, inner, inner]
        aliases = {}
        if out is not None:
            ins.append(out)
            maps.append(None)
            aliases = {5: 0}
        return call(
            functools.partial(fresh_kernel, replicas=pairs), scalars((me ^ k) * pairs + core), ins, maps,
            (jax.ShapeDtypeStruct((rows, width), local.dtype),), (halves,), tile, width, (pairs, steps), aliases,
            16 * area)[0]

    def update_block(piece, total, state):
        k, skip, steps, _, tile, area = geometry(piece, 128)
        column = lambda i, p: (skip + i, p[0])
        ins, maps = [total, weights, momentum], [plain, column, column]
        aliases = {}
        if state is not None:
            ins += list(state)
            maps += [None, None]
            aliases = {4: 0, 5: 1}
        shape = jax.ShapeDtypeStruct(weights.shape, weights.dtype)
        return call(
            functools.partial(update_kernel, replicas=pairs), scalars(me ^ k), ins, maps,
            (shape, shape), (column, column), tile, width, (steps,), aliases, 18 * area)

    send_backs, send_totals, take_backs, take_totals = plan(shards, owned)
    theirs = swap(local)
    backs, totals = {}, {}
    for piece in send_backs:
        backs[piece] = send(back_term(piece), piece[0])
    for piece in send_totals:
        totals[piece] = send(sum_block(piece, theirs), piece[0])
    mine = (0, 0, owned, 0)
    backs[mine] = back_term(mine)
    totals[mine] = sum_block(mine, theirs)
    whole, state = None, None
    for piece in [mine] + take_backs:
        other = swap(backs[piece])
        whole = fresh_block(piece, theirs, backs[piece], other, whole)
    for piece in [mine] + take_totals:
        state = update_block(piece, totals[piece], state)
    return whole, state[0], state[1]


def plain_exchange(local, weights, momentum):
    rows, width = local.shape
    shards = lax.axis_size("shard")
    pairs = lax.axis_size("rep")
    owned = weights.shape[0]
    parts = local.reshape(shards, pairs, owned, width)
    total = lax.psum_scatter(
        parts.astype(jnp.float32).astype(jnp.bfloat16), "rep", scatter_dimension=1, tiled=True
    ).reshape(shards * owned, width)
    total = lax.all_to_all(total, "shard", split_axis=0, concat_axis=1, tiled=True).astype(jnp.float32)
    delta = weights - total / jnp.float32(pairs)
    new_momentum = momentum_decay * momentum + delta
    new_global = weights - outer_rate * (delta + momentum_decay * new_momentum)
    fresh = new_global.astype(jnp.bfloat16)
    spread = lax.all_to_all(fresh, "shard", split_axis=1, concat_axis=0, tiled=True)
    whole = lax.all_gather(
        spread.reshape(shards, 1, owned, width), "rep", axis=1, tiled=True
    ).reshape(rows, width)
    return whole, new_global, new_momentum


def on_device(replica_weights, global_weights, momentum):
    local = replica_weights[0]
    shards, pairs = lax.axis_size("shard"), lax.axis_size("rep")
    fits = local.shape[1] % 128 == 0 and global_weights.shape[0] % 16 == 0
    even = shards >= 4 and shards & (shards - 1) == 0 and pairs == 2
    if not (fits and even):
        return plain_exchange(local, global_weights, momentum)
    return pipelined(local, global_weights, momentum)


def solution(mesh):
    placed = (
        P(("grp", "rep"), None, "shard"),
        P(("grp", "shard", "rep"), None),
        P(("grp", "shard", "rep"), None),
    )
    return jax.shard_map(
        on_device,
        mesh=mesh,
        in_specs=placed,
        out_specs=(
            P("grp", "shard"),
            P(("grp", "shard", "rep"), None),
            P(("grp", "shard", "rep"), None),
        ),
        check_vma=False,
    )
```

```python
import functools
import math

import jax
import jax.numpy as jnp
from jax import lax
from jax.experimental import pallas as pl
from jax.experimental.pallas import tpu as pltpu
from jax.sharding import PartitionSpec as P


outer_rate = 0.7
momentum_decay = 0.9


vmem_limit = 16 * 1024 * 1024
small = 1 << 20


def in_hbm(x):
    return pltpu.with_memory_space_constraint(x, pltpu.HBM)


def call(kernel, place, ins, in_maps, outs, out_maps, tile, width, grid, aliases, bytes_moved):
    any_space = pl.BlockSpec(memory_space=pl.ANY)
    return pl.pallas_call(
        kernel,
        grid_spec=pltpu.PrefetchScalarGridSpec(
            num_scalar_prefetch=1,
            grid=grid,
            in_specs=[any_space if m is None else pl.BlockSpec((tile, width), m) for m in in_maps],
            out_specs=[pl.BlockSpec((tile, width), m) for m in out_maps],
        ),
        out_shape=outs,
        input_output_aliases=aliases,
        compiler_params=pltpu.CompilerParams(vmem_limit_bytes=vmem_limit),
        cost_estimate=pl.CostEstimate(flops=bytes_moved, bytes_accessed=bytes_moved, transcendentals=0),
    )(place, *(x if x.size < small else in_hbm(x) for x in ins))


def back_term_kernel(place, weights, momentum, out):
    keep = 1.0 - outer_rate * (1.0 + momentum_decay)
    carry = outer_rate * momentum_decay * momentum_decay
    out[...] = (keep * weights[...] - carry * momentum[...]).astype(out.dtype)


def sum_kernel(place, mine, theirs, out):
    out[...] = (mine[...].astype(jnp.float32) + theirs[...].astype(jnp.float32)).astype(out.dtype)


def fresh_kernel(place, mine, theirs, back, other, *rest, replicas):
    out = rest[-1]
    share = outer_rate * (1.0 + momentum_decay) / replicas
    total = mine[...].astype(jnp.float32) + theirs[...].astype(jnp.float32)
    first = pl.program_id(0) == 0
    term = jnp.where(first, back[...].astype(jnp.float32), other[...].astype(jnp.float32))
    out[...] = (share * total + term).astype(out.dtype)


def update_kernel(place, total, weights, momentum, *rest, replicas):
    new_weights, new_momentum = rest[-2:]
    old = weights[...]
    delta = old - total[...].astype(jnp.float32) * (1.0 / replicas)
    moved = momentum_decay * momentum[...] + delta
    new_momentum[...] = moved
    new_weights[...] = old - outer_rate * (delta + momentum_decay * moved)


def stage_kernel(weights, momentum, old, moment, sems, *, k, row):
    rows, width = old.shape
    place = pl.multiple_of((lax.axis_index("shard") ^ k) * width, 128)
    window = (pl.ds(row, rows), pl.ds(place, width))
    copies = [
        pltpu.make_async_copy(weights.at[window], old, sems.at[0]),
        pltpu.make_async_copy(momentum.at[window], moment, sems.at[1]),
    ]
    for copy in copies:
        copy.start()
    for copy in copies:
        copy.wait()


def tail_kernel(total, old, moment, carried, also, new_weights, new_momentum, weight, moved, sems, *, k, row, chunks, replicas):
    rows, width = total.shape
    place = pl.multiple_of((lax.axis_index("shard") ^ k) * width, 128)
    step = rows // chunks
    copies = []
    for c in range(chunks):
        part = pl.ds(c * step, step)
        window = (pl.ds(row + c * step, step), pl.ds(place, width))
        update_kernel(
            None, total.at[part], old.at[part], moment.at[part], weight.at[part], moved.at[part], replicas=replicas)
        copies += [
            pltpu.make_async_copy(weight.at[part], new_weights.at[window], sems.at[0, c]),
            pltpu.make_async_copy(moved.at[part], new_momentum.at[window], sems.at[1, c]),
        ]
        copies[-2].start()
        copies[-1].start()
    for copy in copies:
        copy.wait()


def offsets(shards):
    half = shards // 2
    order, top = [], half // 2
    while top:
        lines = range(2 * top - 1, top - 1, -1)
        order += [2 * j for j in lines] + [2 * j + 1 for j in lines]
        top //= 2
    return order + [1]


def cut(k, owned, sizes):
    unit, out, row = owned // 16, [], 0
    for part, size in enumerate(sizes):
        out.append((k, row, size * unit, part))
        row += size * unit
    return out


def plan(shards, owned):
    order = offsets(shards)
    far = [k for k in order if k >= shards // 2]
    near = [k for k in reversed(order) if k < shards // 2]
    half = len(far) // 2
    late = far[:half] + far[half:][::-1]
    backs = {k: cut(k, owned, first_cut if k == order[0] else (16,)) for k in order}
    totals = {k: cut(k, owned, last_cut if k == late[-1] else (16,)) for k in order}
    flat = lambda pieces, ks: [p for k in ks for p in pieces[k]]
    return (
        flat(backs, order), flat(totals, late + [k for k in order if k not in far]),
        flat(backs, far[:half] + near + far[half:]), flat(totals, near + late),
    )


first_cut = (4, 4, 8)
last_cut = (8, 4, 4)
tail_chunks = 4


def pipelined(local, weights, momentum):
    rows, width = local.shape
    shards = lax.axis_size("shard")
    pairs = lax.axis_size("rep")
    owned = weights.shape[0]
    me = lax.axis_index("shard")
    core = lax.axis_index("rep")

    def swap(x):
        return lax.ppermute(x, "rep", [(i, i ^ 1) for i in range(pairs)])

    def send(x, k):
        return lax.ppermute(x, "shard", [(i, i ^ k) for i in range(shards)])

    def scalars(*values):
        return jnp.stack([jnp.asarray(v, jnp.int32) for v in values])

    def geometry(piece, largest):
        k, row, count, _ = piece
        tile = math.gcd(math.gcd(row, count), largest)
        return k, row // tile, count // tile, owned // tile, tile, count * width

    def block(piece):
        return (jax.ShapeDtypeStruct((piece[2], width), local.dtype),)

    plain = lambda i, p: (i, 0)

    def back_term(piece):
        k, skip, steps, _, tile, area = geometry(piece, 128)
        column = lambda i, p: (skip + i, p[0])
        return call(
            back_term_kernel, scalars(me ^ k), (weights, momentum), (column, column),
            block(piece), (plain,), tile, width, (steps,), {}, 10 * area)[0]

    def sum_block(piece, theirs):
        k, skip, steps, per, tile, area = geometry(piece, 128)
        rowed = lambda i, p: (p[0] * per + skip + i, 0)
        return call(
            sum_kernel, scalars((me ^ k) * pairs + core), (local, theirs), (rowed, rowed),
            block(piece), (plain,), tile, width, (steps,), {}, 6 * area)[0]

    def fresh_block(piece, theirs, back, other, out):
        k, skip, steps, per, tile, area = geometry(piece, owned)
        halves = lambda h, i, p: ((p[0] ^ h) * per + skip + i, 0)
        inner = lambda h, i, p: (i, 0)
        ins, maps = [local, theirs, back, other], [halves, halves, inner, inner]
        aliases = {}
        if out is not None:
            ins.append(out)
            maps.append(None)
            aliases = {5: 0}
        return call(
            functools.partial(fresh_kernel, replicas=pairs), scalars((me ^ k) * pairs + core), ins, maps,
            (jax.ShapeDtypeStruct((rows, width), local.dtype),), (halves,), tile, width, (pairs, steps), aliases,
            16 * area)[0]

    def update_block(piece, total, state):
        k, skip, steps, _, tile, area = geometry(piece, 128)
        column = lambda i, p: (skip + i, p[0])
        ins, maps = [total, weights, momentum], [plain, column, column]
        aliases = {}
        if state is not None:
            ins += list(state)
            maps += [None, None]
            aliases = {4: 0, 5: 1}
        shape = jax.ShapeDtypeStruct(weights.shape, weights.dtype)
        return call(
            functools.partial(update_kernel, replicas=pairs), scalars(me ^ k), ins, maps,
            (shape, shape), (column, column), tile, width, (steps,), aliases, 18 * area)

    any_space = pl.BlockSpec(memory_space=pl.ANY)
    vmem = pl.BlockSpec(memory_space=pltpu.VMEM)
    params = pltpu.CompilerParams(vmem_limit_bytes=vmem_limit)

    def cost(moved):
        return pl.CostEstimate(flops=moved, bytes_accessed=moved, transcendentals=0)

    def stage_block(piece):
        k, row, count, _ = piece
        return pl.pallas_call(
            functools.partial(stage_kernel, k=k, row=row),
            in_specs=[any_space] * 2,
            out_specs=(vmem, vmem),
            out_shape=(pltpu.VMEM((count, width), weights.dtype),) * 2,
            scratch_shapes=[pltpu.SemaphoreType.DMA((2,))],
            compiler_params=params,
            cost_estimate=cost(8 * count * width),
            name="stage_block",
        )(in_hbm(weights), in_hbm(momentum))

    def tail_block(piece, total, staged, state):
        k, row, count, _ = piece
        chunks = tail_chunks if count % (16 * tail_chunks) == 0 else 1
        shape = jax.ShapeDtypeStruct(weights.shape, weights.dtype)
        return pl.pallas_call(
            functools.partial(tail_kernel, k=k, row=row, chunks=chunks, replicas=pairs),
            in_specs=[vmem] * 3 + [any_space] * 2,
            out_specs=(any_space, any_space),
            out_shape=(shape, shape),
            scratch_shapes=[pltpu.VMEM((count, width), weights.dtype)] * 2 + [pltpu.SemaphoreType.DMA((2, chunks))],
            input_output_aliases={3: 0, 4: 1},
            compiler_params=params,
            cost_estimate=cost(18 * count * width),
            name="tail_block",
        )(pltpu.with_memory_space_constraint(total, pltpu.VMEM), *staged, *map(in_hbm, state))

    send_backs, send_totals, take_backs, take_totals = plan(shards, owned)
    theirs = swap(local)
    backs, totals = {}, {}
    for piece in send_backs:
        backs[piece] = send(back_term(piece), piece[0])
    for piece in send_totals:
        totals[piece] = send(sum_block(piece, theirs), piece[0])
    mine = (0, 0, owned, 0)
    backs[mine] = back_term(mine)
    totals[mine] = sum_block(mine, theirs)
    last = take_totals[-1]
    staged = stage_block(last)
    whole, state = None, None
    for piece in [mine] + take_backs:
        other = swap(backs[piece])
        whole = fresh_block(piece, theirs, backs[piece], other, whole)
    for piece in [mine] + take_totals:
        if piece == last:
            state = tail_block(piece, totals[piece], staged, state)
        else:
            state = update_block(piece, totals[piece], state)
    return whole, state[0], state[1]


def plain_exchange(local, weights, momentum):
    rows, width = local.shape
    shards = lax.axis_size("shard")
    pairs = lax.axis_size("rep")
    owned = weights.shape[0]
    parts = local.reshape(shards, pairs, owned, width)
    total = lax.psum_scatter(
        parts.astype(jnp.float32).astype(jnp.bfloat16), "rep", scatter_dimension=1, tiled=True
    ).reshape(shards * owned, width)
    total = lax.all_to_all(total, "shard", split_axis=0, concat_axis=1, tiled=True).astype(jnp.float32)
    delta = weights - total / jnp.float32(pairs)
    new_momentum = momentum_decay * momentum + delta
    new_global = weights - outer_rate * (delta + momentum_decay * new_momentum)
    fresh = new_global.astype(jnp.bfloat16)
    spread = lax.all_to_all(fresh, "shard", split_axis=1, concat_axis=0, tiled=True)
    whole = lax.all_gather(
        spread.reshape(shards, 1, owned, width), "rep", axis=1, tiled=True
    ).reshape(rows, width)
    return whole, new_global, new_momentum


def on_device(replica_weights, global_weights, momentum):
    local = replica_weights[0]
    shards, pairs = lax.axis_size("shard"), lax.axis_size("rep")
    fits = local.shape[1] % 128 == 0 and global_weights.shape[0] % 16 == 0
    even = shards >= 4 and shards & (shards - 1) == 0 and pairs == 2
    if not (fits and even):
        return plain_exchange(local, global_weights, momentum)
    return pipelined(local, global_weights, momentum)


def solution(mesh):
    placed = (
        P(("grp", "rep"), None, "shard"),
        P(("grp", "shard", "rep"), None),
        P(("grp", "shard", "rep"), None),
    )
    return jax.shard_map(
        on_device,
        mesh=mesh,
        in_specs=placed,
        out_specs=(
            P("grp", "shard"),
            P(("grp", "shard", "rep"), None),
            P(("grp", "shard", "rep"), None),
        ),
        check_vma=False,
    )
```
